32 devices in a mesh: dp: 4 (over x, y), sp: 8 (over z, core).
Axes of the slice: x: 2, y: 2, z: 4, core: 2. Of those that a mesh axis runs over, the one named last changes fastest.
Arguments:
- x: bfloat16 [32768, 2048], P(('dp', 'sp')), parts along dimension 0
- gain: bfloat16 [2048], replicated
- wq: bfloat16 [2048, 2048], P('sp')
- wk: bfloat16 [2048, 2048], P('sp')
- wv: bfloat16 [2048, 2048], P('sp')
- wo: bfloat16 [2048, 2048], P('sp')
Outputs:
- output: bfloat16 [32768, 2048], P(('dp', 'sp')), parts along dimension 0
There are 4 independent parts. The reference program is written for one: setup_inputs(seed, part) draws one part's arguments, and reference() takes and returns one part's arrays. A program takes and returns all parts, laid end to end along the dimension named above; an argument that names none is the same for every part.
All inputs are finite; a program needn't handle non-finite values.
Results may differ from the reference program's by a relative error of at most 0.012.
Values are sent between devices in bfloat16 or wider.
A program may use at most 2 GiB of HBM per device.

```python
import jax
import jax.numpy as jnp
from jax import lax

ROWS = 8192
D = 2048
HEADS = 8
KV_HEADS = 8
HEAD = 256
THETA = 10000


def setup_inputs(seed: int = 0, part: int = 0) -> dict:
    kx, kn, kq, kk, kv, ko = jax.random.split(jax.random.key(seed), 6)

    def weights(key, rows, columns):
        return jax.random.normal(key, (rows, columns), jnp.float32) * rows**-0.5

    drawn = {
        "x": jax.random.normal(jax.random.fold_in(kx, part), (ROWS, D), jnp.float32),
        "gain": 1 + 0.1 * jax.random.normal(kn, (D,), jnp.float32),
        "wq": 2 * weights(kq, D, HEADS * HEAD),
        "wk": 2 * weights(kk, D, KV_HEADS * HEAD),
        "wv": 4 * weights(kv, D, KV_HEADS * HEAD),
        "wo": weights(ko, HEADS * HEAD, D),
    }
    return {k: v.astype(jnp.bfloat16) for k, v in drawn.items()}


def normed(x, gain):
    wide = x.astype(jnp.float32)
    scale = lax.rsqrt(jnp.mean(wide * wide, -1, keepdims=True) + 1e-6)
    return (wide * scale * gain.astype(jnp.float32)).astype(jnp.bfloat16)


def turned(t, place, theta):
    half = t.shape[-1] // 2
    angle = place.astype(jnp.float32)[:, None] * theta ** (-jnp.arange(half, dtype=jnp.float32) / half)
    cos, sin = jnp.cos(angle)[:, None], jnp.sin(angle)[:, None]
    a, b = t[..., :half].astype(jnp.float32), t[..., half:].astype(jnp.float32)
    return jnp.concatenate([a * cos - b * sin, b * cos + a * sin], -1).astype(jnp.bfloat16)


def matmul(a, w):
    return jnp.dot(a, w, preferred_element_type=jnp.float32).astype(jnp.bfloat16)


def einsum(form, a, b):
    return jnp.einsum(form, a.astype(jnp.float32), b.astype(jnp.float32))


def attention(q, k, v):
    scores = einsum("tgsd,ugd->gstu", q, k) * q.shape[-1] ** -0.5
    token = jnp.arange(q.shape[0])
    scores = jnp.where(token[:, None] >= token, scores, -jnp.inf)
    weights = jax.nn.softmax(scores, -1).astype(jnp.bfloat16)
    return einsum("gstu,ugd->tgsd", weights, v).astype(jnp.bfloat16)


def reference(x, gain, wq, wk, wv, wo):
    a, place = normed(x, gain), jnp.arange(ROWS)
    q = turned(matmul(a, wq).reshape(ROWS, HEADS, HEAD), place, THETA).reshape(ROWS, KV_HEADS, -1, HEAD)
    k = turned(matmul(a, wk).reshape(ROWS, KV_HEADS, HEAD), place, THETA)
    v = matmul(a, wv).reshape(ROWS, KV_HEADS, HEAD)
    seen = attention(q, k, v).reshape(ROWS, HEADS * HEAD)
    return (x.astype(jnp.float32) + jnp.dot(seen, wo, preferred_element_type=jnp.float32)).astype(jnp.bfloat16)
```

```python
import functools

import jax
import jax.numpy as jnp
from jax import lax
from jax.experimental import pallas as pl
from jax.experimental.pallas import tpu as pltpu
from jax.sharding import PartitionSpec as P


NEG = -1e30
HIDDEN = 2 * NEG
LOG2E = 1.4426950408889634
VMEM = 60 * 2**20
STRIP = 512
BLOCK_Q, BLOCK_K = 512, 1024
HEAD = 256
THETA = 10000
D = 2048
SHARD = 256
PLANES = 4
SLOTS = 4
FIRST = 512
CHUNKS = (512, 512)


def _dot(a, b, ca, cb):
    return lax.dot_general(a, b, (((ca,), (cb,)), ((), ())), preferred_element_type=jnp.float32)


def _flash(pos_ref, q_ref, *rest, pieces_of_keys, causal, start, last, scale, bq, bk):
    pairs, rest = [(rest[2 * n], rest[2 * n + 1]) for n in range(pieces_of_keys)], rest[2 * pieces_of_keys :]
    if not start:
        mix_in, top_in, *rest = rest
    if last:
        o_ref, mix_s, top_s = rest
    else:
        mix_s, top_s = rest
    heads = q_ref.shape[0]
    iq = pl.program_id(0)
    e = scale * LOG2E
    wide = min(STRIP, bq)
    pieces = [(i, at) for i in range(heads) for at in range(0, bq, wide)]
    if start:
        top_s[...] = jnp.full(top_s.shape, NEG, jnp.float32)
        mix_s[...] = jnp.zeros(mix_s.shape, jnp.float32)
    else:
        top_s[...] = top_in[...]
        mix_s[...] = mix_in[...]
    ones = jnp.ones((8, bk), q_ref.dtype)

    def block(k_ref, v_ref, j, masked):
        here = pl.ds(pl.multiple_of(j * bk, bk), bk)
        scores = [_dot(k_ref[i, here, :], q_ref[i, at : at + wide, :], 1, 1) for i, at in pieces]
        weights, keeps = [], []
        for (i, at), s in zip(pieces, scores):
            if masked:
                gap = lax.broadcasted_iota(jnp.int32, (bk, wide), 1) - lax.broadcasted_iota(jnp.int32, (bk, wide), 0)
                s = jnp.where(gap >= j * bk - iq * bq - at, s, HIDDEN)
            old = top_s[i, :, at : at + wide]
            top = jnp.maximum(old, s.max(axis=0, keepdims=True))
            top_s[i, :, at : at + wide] = top
            weights.append(jnp.exp2((s - top) * e).astype(q_ref.dtype))
            keeps.append(jnp.exp2((old - top) * e))
        for (i, at), p, keep in zip(pieces, weights, keeps):
            values = jnp.concatenate([v_ref[i, :, here], ones], axis=0)
            mix_s[i, :, at : at + wide] = mix_s[i, :, at : at + wide] * keep + _dot(values, p, 1, 0)

    for k_ref, v_ref in pairs:
        run = lambda masked, k_ref=k_ref, v_ref=v_ref: lambda j, _: block(k_ref, v_ref, j, masked)
        if causal:
            whole = lax.div(iq * bq, bk)
            lax.fori_loop(0, whole, run(False), None)
            lax.fori_loop(whole, lax.div(iq * bq + bq + bk - 1, bk), run(True), None)
        else:
            lax.fori_loop(0, jnp.where(pos_ref[0] > 0, k_ref.shape[1] // bk, 0), run(False), None)
    if last:
        for i in range(heads):
            o_ref[i] = (mix_s[i, :HEAD, :] * (1 / mix_s[i, HEAD : HEAD + 1, :])).T.astype(o_ref.dtype)


def flash(q, keys, state, seen, *, causal=False, last=False):
    heads, sq, d = q.shape
    bq, bk = BLOCK_Q, min([BLOCK_K] + [k.shape[1] for k, _ in keys])
    sk = sum(k.shape[1] for k, _ in keys)
    given, specs = [q], [pl.BlockSpec((heads, bq, d), lambda i, _: (0, i, 0))]
    for pair in keys:
        given += pair
        specs += [pl.BlockSpec(t.shape, lambda i, _: (0, 0, 0)) for t in pair]
    n = len(given)
    state_specs = [pl.BlockSpec((heads, d + 8, bq), lambda i, _: (0, 0, i)), pl.BlockSpec((heads, 1, bq), lambda i, _: (0, 0, i))]
    state_shapes = [jax.ShapeDtypeStruct((heads, d + 8, sq), jnp.float32), jax.ShapeDtypeStruct((heads, 1, sq), jnp.float32)]
    if state is not None:
        given += list(state)
        specs += state_specs
    if last:
        out_specs, out_shape = [specs[0]], [jax.ShapeDtypeStruct(q.shape, q.dtype)]
        scratch = [pltpu.VMEM((heads, d + 8, bq), jnp.float32), pltpu.VMEM((heads, 1, bq), jnp.float32)]
    else:
        out_specs, out_shape, scratch = state_specs, state_shapes, []
    return pl.pallas_call(
        functools.partial(_flash, pieces_of_keys=len(keys), causal=causal, start=state is None, last=last, scale=d**-0.5, bq=bq, bk=bk),
        grid_spec=pltpu.PrefetchScalarGridSpec(
            num_scalar_prefetch=1, grid=(sq // bq,), in_specs=specs, out_specs=out_specs, scratch_shapes=scratch
        ),
        out_shape=out_shape,
        input_output_aliases={n + 1: 0, n + 2: 1} if state is not None and not last else {},
        compiler_params=pltpu.CompilerParams(dimension_semantics=("arbitrary",), vmem_limit_bytes=VMEM),
        cost_estimate=pl.CostEstimate(
            flops=4 * heads * sq * sk * d // (2 if causal else 1),
            transcendentals=heads * sq * sk,
            bytes_accessed=2 * heads * d * (sq + 2 * sk),
        ),
    )(jnp.reshape(seen, (1,)).astype(jnp.int32), *given)


MESH = pl.DeviceIdType.MESH


def _fetch(*refs):
    n = len(refs) - 14
    x_ref, shards, w_ref, here_ref, below_ref = refs[0], refs[1 : n + 1], *refs[n + 1 : n + 4]
    mine, x_s, load_sem, store_sem, swap_sem, z_send, z_recv, xy_send, xy_recv, x_sem = refs[n + 4 :]
    index, g = lax.axis_index("sp"), lax.axis_index("dp")
    z, c = index // 2, index % 2
    rows = lambda plane, core: pl.ds(pl.multiple_of(512 * plane + 256 * core, 256), SHARD)
    part = pl.ds(pl.multiple_of(HEAD * g, HEAD), HEAD)
    line = lambda k: lax.rem(z + k, PLANES)

    loads = [pltpu.make_async_copy(shards[t], mine.at[t], load_sem.at[t]) for t in range(n)]
    loads.append(pltpu.make_async_copy(x_ref, x_s, load_sem.at[n]))
    for load in loads:
        load.start()
    barrier = pltpu.get_barrier_semaphore()
    partners = [(g, 2 * line(k) + core) for k in range(1, PLANES) for core in range(2)] + [(g, 2 * z + 1 - c), (g ^ 1, index), (g ^ 2, index)]
    for device in partners:
        pl.semaphore_signal(barrier, inc=1, device_id=device, device_id_type=MESH)
    pl.semaphore_wait(barrier, len(partners))

    def remote(src, dst, send, recv, device):
        return pltpu.make_async_remote_copy(src_ref=src, dst_ref=dst, send_sem=send, recv_sem=recv, device_id=device, device_id_type=MESH)

    def along(t, k, core):
        cols = pl.ds(pl.multiple_of(4 * HEAD * core + HEAD * g, HEAD), HEAD)
        return remote(mine.at[t, :, cols], w_ref.at[t, rows(z, c), part], z_send.at[t, k - 1, core], z_recv.at[t, k - 1, c], (g, 2 * line(k) + core))

    def arrived(t, k, s):
        spot = w_ref.at[t, rows(line(PLANES - k), s), part]
        remote(spot, spot, z_send.at[t, k - 1, 0], z_recv.at[t, k - 1, s], (g, 2 * line(k))).wait_recv()

    def across(t, k, s, quarter, to, slot):
        q = pl.ds(pl.multiple_of(HEAD * (g ^ quarter), HEAD), HEAD)
        spot = w_ref.at[t, rows(line(PLANES - k), s), q]
        return remote(spot, spot, xy_send.at[t, k - 1, s, slot], xy_recv.at[t, k - 1, s, slot], (g ^ to, index))

    sent, stores = [], []
    pieces = [(t, k, s) for t in range(n) for k in range(1, PLANES) for s in range(2)]
    for t in range(n):
        loads[t].wait()
        for k in range(1, PLANES):
            for core in range(2):
                sent.append(along(t, k, core))
                sent[-1].start()
        theirs = pl.ds(pl.multiple_of(4 * HEAD * (1 - c), 4 * HEAD), 4 * HEAD)
        ours = pl.ds(pl.multiple_of(4 * HEAD * c, 4 * HEAD), 4 * HEAD)
        other = remote(mine.at[t, :, theirs], w_ref.at[t, rows(z, c), :], swap_sem.at[t, 0], swap_sem.at[t, 1], (g, 2 * z + 1 - c))
        other.start()
        sent.append(other)
        stores.append(pltpu.make_async_copy(mine.at[t, :, ours], w_ref.at[t, rows(z, c), :], store_sem.at[t]))
        stores[-1].start()

    loads[n].wait()
    other = (g, 2 * z + 1 - c)
    stores.append(pltpu.make_async_copy(x_s, here_ref.at[c], store_sem.at[n]))
    stores[-1].start()
    sent.append(remote(x_s, here_ref.at[c], x_sem.at[0, 0], x_sem.at[0, 1], other))
    sent[-1].start()
    sent.append(remote(x_s.at[pl.ds(0, FIRST)], below_ref.at[c], x_sem.at[1, 0], x_sem.at[1, 1], (g, 2 * line(1) + c)))
    sent[-1].start()

    def relay(t, k, s):
        came, to = (2, 1) if s == 0 else (1, 2)
        across(t, k, s, came, came, came - 1).wait_recv()
        sent.append(across(t, k, s, came, to, 2))
        sent[-1].start()

    lag = 2
    for i, piece in enumerate(pieces):
        arrived(*piece)
        for to in (1, 2):
            sent.append(across(*piece, 0, to, to - 1))
            sent[-1].start()
        if i >= lag:
            relay(*pieces[i - lag])
    for piece in pieces[len(pieces) - lag :]:
        relay(*piece)
    for t, k, s in pieces:
        stays = 1 if s == 0 else 2
        across(t, k, s, stays, stays, stays - 1).wait_recv()
        across(t, k, s, 3, 3, 2).wait_recv()
    for t in range(n):
        spot = w_ref.at[t, rows(z, 1 - c), :]
        remote(spot, spot, swap_sem.at[t, 0], swap_sem.at[t, 1], (g, 2 * z + 1 - c)).wait_recv()
        stores[t].wait()
    stores[n].wait()
    remote(here_ref.at[1 - c], here_ref.at[1 - c], x_sem.at[0, 0], x_sem.at[0, 1], other).wait_recv()
    spot = below_ref.at[c]
    remote(spot, spot, x_sem.at[1, 0], x_sem.at[1, 1], (g, 2 * line(1) + c)).wait_recv()
    sent.append(remote(spot, spot, x_sem.at[2, 0], x_sem.at[2, 1], other))
    sent[-1].start()
    spot = below_ref.at[1 - c]
    remote(spot, spot, x_sem.at[2, 0], x_sem.at[2, 1], other).wait_recv()
    for copy in sent:
        copy.wait_send()


def fetch(x, *shards):
    n = len(shards)
    dma = pltpu.SemaphoreType.DMA
    return pl.pallas_call(
        _fetch,
        in_specs=[pl.BlockSpec(memory_space=pl.ANY)] * (n + 1),
        out_specs=[pl.BlockSpec(memory_space=pl.ANY)] * 3,
        out_shape=[
            jax.ShapeDtypeStruct((n, D, D // 2), jnp.bfloat16),
            jax.ShapeDtypeStruct((2, *x.shape), jnp.bfloat16),
            jax.ShapeDtypeStruct((2, FIRST, D), jnp.bfloat16),
        ],
        scratch_shapes=[
            pltpu.VMEM((n, SHARD, D), jnp.bfloat16),
            pltpu.VMEM(x.shape, jnp.bfloat16),
            dma((n + 1,)),
            dma((n + 1,)),
            dma((n, 2)),
            dma((n, 3, 2)),
            dma((n, 3, 2)),
            dma((n, 3, 2, 3)),
            dma((n, 3, 2, 3)),
            dma((3, 2)),
        ],
        compiler_params=pltpu.CompilerParams(collective_id=0, has_side_effects=True, vmem_limit_bytes=VMEM),
        cost_estimate=pl.CostEstimate(flops=10**11, transcendentals=0, bytes_accessed=10**7),
    )(x, *shards)


def _project(*refs, parts, blocks, turned):
    *xs, gain_ref, cos_ref, sin_ref, w_ref = refs[: parts + 4]
    outs = refs[parts + 4 :]
    wide = xs[0][...] if parts == 1 else jnp.where(pl.program_id(0) < blocks, xs[0][...], xs[1][...])
    wide = wide.astype(jnp.float32)
    scale = lax.rsqrt(jnp.mean(wide * wide, -1, keepdims=True) + 1e-6)
    a = (wide * scale * gain_ref[...].astype(jnp.float32)).astype(jnp.bfloat16)
    cos, sin = cos_ref[...], sin_ref[...]
    half = HEAD // 2
    for t, o in enumerate(outs):
        y = _dot(a, w_ref[t], 1, 0).astype(jnp.bfloat16)
        for m in range(SLOTS):
            part = y[:, m * HEAD : (m + 1) * HEAD]
            if turned[t]:
                lo, hi = part[:, :half].astype(jnp.float32), part[:, half:].astype(jnp.float32)
                o[m, :, :half] = (lo * cos - hi * sin).astype(jnp.bfloat16)
                o[m, :, half:] = (hi * cos + lo * sin).astype(jnp.bfloat16)
            else:
                o[m] = part.T


def project(xs, gain, cos, sin, w, turned):
    part = xs[0].shape[0]
    rows, tb, n = part * len(xs), min(512, part), len(turned)
    blocks = part // tb
    if len(xs) == 1:
        specs = [pl.BlockSpec((tb, D), lambda i: (i, 0))]
    else:
        specs = [pl.BlockSpec((tb, D), lambda i: (jnp.minimum(i, blocks - 1), 0)), pl.BlockSpec((tb, D), lambda i: (jnp.maximum(i - blocks, 0), 0))]
    size = SLOTS * rows * HEAD
    return pl.pallas_call(
        functools.partial(_project, parts=len(xs), blocks=blocks, turned=turned),
        grid=(rows // tb,),
        in_specs=specs
        + [
            pl.BlockSpec((1, D), lambda i: (0, 0)),
            pl.BlockSpec((tb, HEAD // 2), lambda i: (i, 0)),
            pl.BlockSpec((tb, HEAD // 2), lambda i: (i, 0)),
            pl.BlockSpec((n, D, D // 2), lambda i: (0, 0, 0), pipeline_mode=pl.Buffered(1)),
        ],
        out_specs=[pl.BlockSpec((SLOTS, tb, HEAD), lambda i: (0, i, 0)) if t else pl.BlockSpec((SLOTS, HEAD, tb), lambda i: (0, 0, i)) for t in turned],
        out_shape=[jax.ShapeDtypeStruct((SLOTS, rows, HEAD) if t else (SLOTS, HEAD, rows), jnp.bfloat16) for t in turned],
        compiler_params=pltpu.CompilerParams(dimension_semantics=("arbitrary",), vmem_limit_bytes=VMEM),
        cost_estimate=pl.CostEstimate(flops=2 * size * D * n, transcendentals=rows, bytes_accessed=2 * (rows * D + n * D * D // 2 + n * size)),
    )(*xs, gain, cos, sin, w)


def _finish(at_ref, x_ref, mine_ref, theirs_ref, w_ref, y_ref, a_s):
    core = at_ref[0]
    for half, ref in ((core, mine_ref), (1 - core, theirs_ref)):
        for m in range(SLOTS):
            a_s[:, pl.ds(pl.multiple_of((4 * half + m) * HEAD, HEAD), HEAD)] = ref[m]
    a = a_s[...]
    wide = D // SLOTS
    for g in range(SLOTS):
        cols = slice(g * wide, (g + 1) * wide)
        y_ref[:, cols] = (x_ref[:, cols].astype(jnp.float32) + _dot(a, w_ref[g], 1, 0)).astype(jnp.bfloat16)


def finish(x, mine, theirs, w, core):
    rows, tb = x.shape[0], 256
    heads = pl.BlockSpec((SLOTS, tb, HEAD), lambda i, _: (0, i, 0))
    return pl.pallas_call(
        _finish,
        grid_spec=pltpu.PrefetchScalarGridSpec(
            num_scalar_prefetch=1,
            grid=(rows // tb,),
            in_specs=[pl.BlockSpec((tb, D), lambda i, _: (i, 0)), heads, heads, pl.BlockSpec((SLOTS, D, D // SLOTS), lambda i, _: (0, 0, 0))],
            out_specs=pl.BlockSpec((tb, D), lambda i, _: (i, 0)),
            scratch_shapes=[pltpu.VMEM((tb, D), jnp.bfloat16)],
        ),
        out_shape=jax.ShapeDtypeStruct(x.shape, x.dtype),
        compiler_params=pltpu.CompilerParams(dimension_semantics=("arbitrary",), vmem_limit_bytes=VMEM),
        cost_estimate=pl.CostEstimate(flops=2 * rows * D * D, transcendentals=0, bytes_accessed=2 * (3 * x.size + D * D)),
    )(jnp.reshape(core, (1,)).astype(jnp.int32), x, mine, theirs, w)


def swap(t):
    return lax.ppermute(t, "sp", [(i, i ^ 1) for i in range(2 * PLANES)])


def up(t, step):
    return lax.ppermute(t, "sp", [(i, i + 2) for i in range(2 * (step - 1), 2 * (PLANES - 1))])


def solution(mesh):
    def step(x, gain, wq, wk, wv, wo):
        own = x.shape[0]
        index, group = lax.axis_index("sp"), lax.axis_index("dp")
        z, core = index // 2, index % 2
        gain = gain.reshape(1, D)
        freq = THETA ** (-jnp.arange(HEAD // 2, dtype=jnp.float32) / (HEAD // 2))

        def angles(chip, first, rows, core):
            place = (chip * 2 + (core ^ jnp.arange(2)[:, None])) * own + first + jnp.arange(rows)[None, :]
            angle = place.reshape(-1).astype(jnp.float32)[:, None] * freq
            return jnp.cos(angle), jnp.sin(angle)

        def after(t, *others):
            return lax.optimization_barrier((t, *others))[0]

        w, here, below = fetch(x, wk, wv, wq)
        sizes = list(zip([sum(CHUNKS[:n]) for n in range(len(CHUNKS))], CHUNKS))
        turns = [[angles(z - s, a, n, 0 if s == 1 and a == 0 else core) for a, n in sizes] for s in range(1, PLANES)]

        def both(t):
            return [t, swap(t)]

        count = len(CHUNKS)
        held = [lax.dynamic_index_in_dim(below, core, keepdims=False)] + [up(after(x[a : a + m], w), 1) for n, (a, m) in enumerate(sizes) if n]
        onward = [up(held[0], 2)]
        k, v, q = project([after(here.reshape(-1, D), held[0])], gain, *angles(z, 0, own, 0), w, (True, False, True))
        state = flash(q, [(k, v)], None, 1, causal=True)
        quarter = lax.dynamic_slice_in_dim(after(wo, state[1]), group * (D // SLOTS), D // SLOTS, axis=1)
        w_out = lax.all_gather(lax.all_gather(quarter, "sp", axis=0, tiled=True), "dp", axis=0)
        done = wait = state[1]
        for s in range(1, PLANES):
            seen, keys = (z >= s).astype(jnp.int32), []
            for n in range(count):
                if s == 1 and n == 0:
                    xs = [after(below.reshape(-1, D), done)]
                else:
                    t = after(held[n], wait if n == 0 else state[1])
                    if s < PLANES - 1 and not (s == 1 and n == 0):
                        onward.append(up(t, s + 1))
                    xs = both(t)
                    xs[0] = after(xs[0], done)
                keys.append(project(xs, gain, *turns[s - 1][n], w, (True, False)))
                wait = done = keys[-1][0]
                end = n == count - 1
                if end or s == PLANES - 1:
                    state = flash(q, keys, state, seen, last=end and s == PLANES - 1)
                    keys, done = [], state[1] if len(state) > 1 else None
            held, onward = onward, []
        seen = state[0]
        rows = lambda c: lax.dynamic_slice_in_dim(seen, c * own, own, axis=1)
        return finish(x, rows(core), swap(rows(1 - core)), w_out, core)

    tokens, whole = P(("dp", "sp"), None), P("sp", None)
    return jax.shard_map(
        step,
        mesh=mesh,
        in_specs=(tokens, P(None), whole, whole, whole, whole),
        out_specs=tokens,
        check_vma=False,
    )
```

```python
import functools

import jax
import jax.numpy as jnp
from jax import lax
from jax.experimental import pallas as pl
from jax.experimental.pallas import tpu as pltpu
from jax.sharding import PartitionSpec as P


NEG = -1e30
HIDDEN = 2 * NEG
LOG2E = 1.4426950408889634
VMEM = 60 * 2**20
STRIP = 512
BLOCK_Q, BLOCK_K = 512, 1024
HEAD = 256
THETA = 10000
D = 2048
SHARD = 256
PLANES = 4
SLOTS = 4
FIRST = 512
CHUNKS = (512, 512)


def _dot(a, b, ca, cb):
    return lax.dot_general(a, b, (((ca,), (cb,)), ((), ())), preferred_element_type=jnp.float32)


def _flash(pos_ref, q_ref, *rest, pieces_of_keys, causal, start, part, scale, bq, bk):
    pairs, rest = [(rest[2 * n], rest[2 * n + 1]) for n in range(pieces_of_keys)], rest[2 * pieces_of_keys :]
    if not start:
        mix_in, top_in, *rest = rest
    if part:
        o_ref, stat_ref, mix_s, top_s = rest
    else:
        mix_s, top_s = rest
    heads = q_ref.shape[0]
    iq = pl.program_id(0)
    e = scale * LOG2E
    wide = min(STRIP, bq)
    pieces = [(i, at) for i in range(heads) for at in range(0, bq, wide)]
    if start:
        top_s[...] = jnp.full(top_s.shape, NEG, jnp.float32)
        mix_s[...] = jnp.zeros(mix_s.shape, jnp.float32)
    else:
        top_s[...] = top_in[...]
        mix_s[...] = mix_in[...]
    ones = jnp.ones((8, bk), q_ref.dtype)

    def block(k_ref, v_ref, j, masked):
        here = pl.ds(pl.multiple_of(j * bk, bk), bk)
        scores = [_dot(k_ref[i, here, :], q_ref[i, at : at + wide, :], 1, 1) for i, at in pieces]
        weights, keeps = [], []
        for (i, at), s in zip(pieces, scores):
            if masked:
                gap = lax.broadcasted_iota(jnp.int32, (bk, wide), 1) - lax.broadcasted_iota(jnp.int32, (bk, wide), 0)
                s = jnp.where(gap >= j * bk - iq * bq - at, s, HIDDEN)
            old = top_s[i, :, at : at + wide]
            top = jnp.maximum(old, s.max(axis=0, keepdims=True))
            top_s[i, :, at : at + wide] = top
            weights.append(jnp.exp2((s - top) * e).astype(q_ref.dtype))
            keeps.append(jnp.exp2((old - top) * e))
        for (i, at), p, keep in zip(pieces, weights, keeps):
            values = jnp.concatenate([v_ref[i, :, here], ones], axis=0)
            mix_s[i, :, at : at + wide] = mix_s[i, :, at : at + wide] * keep + _dot(values, p, 1, 0)

    for k_ref, v_ref in pairs:
        run = lambda masked, k_ref=k_ref, v_ref=v_ref: lambda j, _: block(k_ref, v_ref, j, masked)
        if causal:
            whole = lax.div(iq * bq, bk)
            lax.fori_loop(0, whole, run(False), None)
            lax.fori_loop(whole, lax.div(iq * bq + bq + bk - 1, bk), run(True), None)
        else:
            lax.fori_loop(0, jnp.where(pos_ref[0] > 0, k_ref.shape[1] // bk, 0), run(False), None)
    if part:
        total = mix_s[:, HEAD : HEAD + 1, :]
        o_ref[...] = (mix_s[:, :HEAD, :] * (1 / total)).astype(o_ref.dtype)
        stat_ref[...] = top_s[...] + jnp.log2(total) * (1 / e)


def _merge(mix_ref, top_ref, *refs, scale, blocks):
    oa_ref, ob_ref, sa_ref, sb_ref, o_ref = refs
    e = scale * LOG2E
    early = pl.program_id(0) < blocks
    top, stat = top_ref[...], jnp.where(early, sa_ref[...], sb_ref[...])
    high = jnp.maximum(top, stat)
    one, two = jnp.exp2((top - high) * e), jnp.exp2((stat - high) * e)
    share = 1 / (mix_ref[:, HEAD : HEAD + 1, :] * one + two)
    one, two = one * share, two * share
    for i in range(o_ref.shape[0]):
        far = jnp.where(early, oa_ref[i], ob_ref[i]).astype(jnp.float32)
        o_ref[i] = (mix_ref[i, :HEAD, :] * one[i] + far * two[i]).T.astype(o_ref.dtype)


def merge(state, outs, stats):
    mix, top = state
    heads, _, sq = mix.shape
    bq = BLOCK_Q
    blocks = outs[0].shape[2] // bq
    first, second = lambda i: (0, 0, jnp.minimum(i, blocks - 1)), lambda i: (0, 0, jnp.maximum(i - blocks, 0))
    return pl.pallas_call(
        functools.partial(_merge, scale=HEAD**-0.5, blocks=blocks),
        grid=(sq // bq,),
        in_specs=[
            pl.BlockSpec((heads, HEAD + 8, bq), lambda i: (0, 0, i)),
            pl.BlockSpec((heads, 1, bq), lambda i: (0, 0, i)),
            pl.BlockSpec((heads, HEAD, bq), first),
            pl.BlockSpec((heads, HEAD, bq), second),
            pl.BlockSpec((heads, 1, bq), first),
            pl.BlockSpec((heads, 1, bq), second),
        ],
        out_specs=pl.BlockSpec((heads, bq, HEAD), lambda i: (0, i, 0)),
        out_shape=jax.ShapeDtypeStruct((heads, sq, HEAD), jnp.bfloat16),
        compiler_params=pltpu.CompilerParams(dimension_semantics=("arbitrary",), vmem_limit_bytes=VMEM),
        cost_estimate=pl.CostEstimate(flops=4 * mix.size, transcendentals=2 * top.size, bytes_accessed=4 * mix.size + 4 * heads * sq * HEAD),
    )(mix, top, *outs, *stats)


def flash(q, keys, state, seen, *, causal=False, part=False):
    heads, sq, d = q.shape
    bq, bk = BLOCK_Q, min([BLOCK_K] + [k.shape[1] for k, _ in keys])
    sk = sum(k.shape[1] for k, _ in keys)
    given, specs = [q], [pl.BlockSpec((heads, bq, d), lambda i, _: (0, i, 0))]
    for pair in keys:
        given += pair
        specs += [pl.BlockSpec(t.shape, lambda i, _: (0, 0, 0)) for t in pair]
    n = len(given)
    state_specs = [pl.BlockSpec((heads, d + 8, bq), lambda i, _: (0, 0, i)), pl.BlockSpec((heads, 1, bq), lambda i, _: (0, 0, i))]
    state_shapes = [jax.ShapeDtypeStruct((heads, d + 8, sq), jnp.float32), jax.ShapeDtypeStruct((heads, 1, sq), jnp.float32)]
    if state is not None:
        given += list(state)
        specs += state_specs
    if part:
        out_specs = [pl.BlockSpec((heads, d, bq), lambda i, _: (0, 0, i)), state_specs[1]]
        out_shape = [jax.ShapeDtypeStruct((heads, d, sq), q.dtype), state_shapes[1]]
        scratch = [pltpu.VMEM((heads, d + 8, bq), jnp.float32), pltpu.VMEM((heads, 1, bq), jnp.float32)]
    else:
        out_specs, out_shape, scratch = state_specs, state_shapes, []
    return pl.pallas_call(
        functools.partial(_flash, pieces_of_keys=len(keys), causal=causal, start=state is None, part=part, scale=d**-0.5, bq=bq, bk=bk),
        grid_spec=pltpu.PrefetchScalarGridSpec(
            num_scalar_prefetch=1, grid=(sq // bq,), in_specs=specs, out_specs=out_specs, scratch_shapes=scratch
        ),
        out_shape=out_shape,
        input_output_aliases={n + 1: 0, n + 2: 1} if state is not None else {},
        compiler_params=pltpu.CompilerParams(dimension_semantics=("arbitrary",), vmem_limit_bytes=VMEM),
        cost_estimate=pl.CostEstimate(
            flops=4 * heads * sq * sk * d // (2 if causal else 1),
            transcendentals=heads * sq * sk,
            bytes_accessed=2 * heads * d * (sq + 2 * sk),
        ),
    )(jnp.reshape(seen, (1,)).astype(jnp.int32), *given)


MESH = pl.DeviceIdType.MESH


def _fetch(*refs):
    n = len(refs) - 14
    x_ref, shards, w_ref, here_ref, below_ref = refs[0], refs[1 : n + 1], *refs[n + 1 : n + 4]
    mine, x_s, load_sem, store_sem, swap_sem, z_send, z_recv, xy_send, xy_recv, x_sem = refs[n + 4 :]
    index, g = lax.axis_index("sp"), lax.axis_index("dp")
    z, c = index // 2, index % 2
    rows = lambda plane, core: pl.ds(pl.multiple_of(512 * plane + 256 * core, 256), SHARD)
    part = pl.ds(pl.multiple_of(HEAD * g, HEAD), HEAD)
    line = lambda k: lax.rem(z + k, PLANES)

    loads = [pltpu.make_async_copy(shards[t], mine.at[t], load_sem.at[t]) for t in range(n)]
    loads.append(pltpu.make_async_copy(x_ref, x_s, load_sem.at[n]))
    for load in loads:
        load.start()
    barrier = pltpu.get_barrier_semaphore()
    partners = [(g, 2 * line(k) + core) for k in range(1, PLANES) for core in range(2)] + [(g, 2 * z + 1 - c), (g ^ 1, index), (g ^ 2, index)]
    for device in partners:
        pl.semaphore_signal(barrier, inc=1, device_id=device, device_id_type=MESH)
    pl.semaphore_wait(barrier, len(partners))

    def remote(src, dst, send, recv, device):
        return pltpu.make_async_remote_copy(src_ref=src, dst_ref=dst, send_sem=send, recv_sem=recv, device_id=device, device_id_type=MESH)

    def along(t, k, core):
        cols = pl.ds(pl.multiple_of(4 * HEAD * core + HEAD * g, HEAD), HEAD)
        return remote(mine.at[t, :, cols], w_ref.at[t, rows(z, c), part], z_send.at[t, k - 1, core], z_recv.at[t, k - 1, c], (g, 2 * line(k) + core))

    def arrived(t, k, s):
        spot = w_ref.at[t, rows(line(PLANES - k), s), part]
        remote(spot, spot, z_send.at[t, k - 1, 0], z_recv.at[t, k - 1, s], (g, 2 * line(k))).wait_recv()

    def across(t, k, s, quarter, to, slot):
        q = pl.ds(pl.multiple_of(HEAD * (g ^ quarter), HEAD), HEAD)
        spot = w_ref.at[t, rows(line(PLANES - k), s), q]
        return remote(spot, spot, xy_send.at[t, k - 1, s, slot], xy_recv.at[t, k - 1, s, slot], (g ^ to, index))

    sent, stores = [], []
    pieces = [(t, k, s) for t in range(n) for k in range(1, PLANES) for s in range(2)]
    for t in range(n):
        loads[t].wait()
        for k in range(1, PLANES):
            for core in range(2):
                sent.append(along(t, k, core))
                sent[-1].start()
        theirs = pl.ds(pl.multiple_of(4 * HEAD * (1 - c), 4 * HEAD), 4 * HEAD)
        ours = pl.ds(pl.multiple_of(4 * HEAD * c, 4 * HEAD), 4 * HEAD)
        other = remote(mine.at[t, :, theirs], w_ref.at[t, rows(z, c), :], swap_sem.at[t, 0], swap_sem.at[t, 1], (g, 2 * z + 1 - c))
        other.start()
        sent.append(other)
        stores.append(pltpu.make_async_copy(mine.at[t, :, ours], w_ref.at[t, rows(z, c), :], store_sem.at[t]))
        stores[-1].start()

    loads[n].wait()
    other = (g, 2 * z + 1 - c)
    stores.append(pltpu.make_async_copy(x_s, here_ref.at[c], store_sem.at[n]))
    stores[-1].start()
    sent.append(remote(x_s, here_ref.at[c], x_sem.at[0, 0], x_sem.at[0, 1], other))
    sent[-1].start()
    rise = remote(x_s.at[pl.ds(0, FIRST)], below_ref.at[c], x_sem.at[1, 0], x_sem.at[1, 1], (g, 2 * line(1) + c))
    pl.when(z < PLANES - 1)(rise.start)

    def relay(t, k, s):
        came, to = (2, 1) if s == 0 else (1, 2)
        across(t, k, s, came, came, came - 1).wait_recv()
        sent.append(across(t, k, s, came, to, 2))
        sent[-1].start()

    lag = 2
    for i, piece in enumerate(pieces):
        arrived(*piece)
        for to in (1, 2):
            sent.append(across(*piece, 0, to, to - 1))
            sent[-1].start()
        if i >= lag:
            relay(*pieces[i - lag])
    for piece in pieces[len(pieces) - lag :]:
        relay(*piece)
    for t, k, s in pieces:
        stays = 1 if s == 0 else 2
        across(t, k, s, stays, stays, stays - 1).wait_recv()
        across(t, k, s, 3, 3, 2).wait_recv()
    for t in range(n):
        spot = w_ref.at[t, rows(z, 1 - c), :]
        remote(spot, spot, swap_sem.at[t, 0], swap_sem.at[t, 1], (g, 2 * z + 1 - c)).wait_recv()
        stores[t].wait()
    stores[n].wait()
    remote(here_ref.at[1 - c], here_ref.at[1 - c], x_sem.at[0, 0], x_sem.at[0, 1], other).wait_recv()

    @pl.when(z > 0)
    def _():
        rise.wait_recv()
        spot = below_ref.at[c]
        on = remote(spot, spot, x_sem.at[2, 0], x_sem.at[2, 1], other)
        on.start()
        spot = below_ref.at[1 - c]
        remote(spot, spot, x_sem.at[2, 0], x_sem.at[2, 1], other).wait_recv()
        on.wait_send()

    pl.when(z < PLANES - 1)(rise.wait_send)
    for copy in sent:
        copy.wait_send()


def fetch(x, *shards):
    n = len(shards)
    dma = pltpu.SemaphoreType.DMA
    return pl.pallas_call(
        _fetch,
        in_specs=[pl.BlockSpec(memory_space=pl.ANY)] * (n + 1),
        out_specs=[pl.BlockSpec(memory_space=pl.ANY)] * 3,
        out_shape=[
            jax.ShapeDtypeStruct((n, D, D // 2), jnp.bfloat16),
            jax.ShapeDtypeStruct((2, *x.shape), jnp.bfloat16),
            jax.ShapeDtypeStruct((2, FIRST, D), jnp.bfloat16),
        ],
        scratch_shapes=[
            pltpu.VMEM((n, SHARD, D), jnp.bfloat16),
            pltpu.VMEM(x.shape, jnp.bfloat16),
            dma((n + 1,)),
            dma((n + 1,)),
            dma((n, 2)),
            dma((n, 3, 2)),
            dma((n, 3, 2)),
            dma((n, 3, 2, 3)),
            dma((n, 3, 2, 3)),
            dma((3, 2)),
        ],
        compiler_params=pltpu.CompilerParams(collective_id=0, has_side_effects=True, vmem_limit_bytes=VMEM),
        cost_estimate=pl.CostEstimate(flops=10**11, transcendentals=0, bytes_accessed=10**7),
    )(x, *shards)


def _project(*refs, parts, blocks, turned):
    *xs, gain_ref, cos_ref, sin_ref, w_ref = refs[: parts + 4]
    outs = refs[parts + 4 :]
    wide = xs[0][...] if parts == 1 else jnp.where(pl.program_id(0) < blocks, xs[0][...], xs[1][...])
    wide = wide.astype(jnp.float32)
    scale = lax.rsqrt(jnp.mean(wide * wide, -1, keepdims=True) + 1e-6)
    a = (wide * scale * gain_ref[...].astype(jnp.float32)).astype(jnp.bfloat16)
    cos, sin = cos_ref[...], sin_ref[...]
    half = HEAD // 2
    for t, o in enumerate(outs):
        y = _dot(a, w_ref[t], 1, 0).astype(jnp.bfloat16)
        for m in range(SLOTS):
            part = y[:, m * HEAD : (m + 1) * HEAD]
            if turned[t]:
                lo, hi = part[:, :half].astype(jnp.float32), part[:, half:].astype(jnp.float32)
                o[m, :, :half] = (lo * cos - hi * sin).astype(jnp.bfloat16)
                o[m, :, half:] = (hi * cos + lo * sin).astype(jnp.bfloat16)
            else:
                o[m] = part.T


def project(xs, gain, cos, sin, w, turned):
    part = xs[0].shape[0]
    rows, tb, n = part * len(xs), min(512, part), len(turned)
    blocks = part // tb
    if len(xs) == 1:
        specs = [pl.BlockSpec((tb, D), lambda i: (i, 0))]
    else:
        specs = [pl.BlockSpec((tb, D), lambda i: (jnp.minimum(i, blocks - 1), 0)), pl.BlockSpec((tb, D), lambda i: (jnp.maximum(i - blocks, 0), 0))]
    size = SLOTS * rows * HEAD
    return pl.pallas_call(
        functools.partial(_project, parts=len(xs), blocks=blocks, turned=turned),
        grid=(rows // tb,),
        in_specs=specs
        + [
            pl.BlockSpec((1, D), lambda i: (0, 0)),
            pl.BlockSpec((tb, HEAD // 2), lambda i: (i, 0)),
            pl.BlockSpec((tb, HEAD // 2), lambda i: (i, 0)),
            pl.BlockSpec((n, D, D // 2), lambda i: (0, 0, 0), pipeline_mode=pl.Buffered(1)),
        ],
        out_specs=[pl.BlockSpec((SLOTS, tb, HEAD), lambda i: (0, i, 0)) if t else pl.BlockSpec((SLOTS, HEAD, tb), lambda i: (0, 0, i)) for t in turned],
        out_shape=[jax.ShapeDtypeStruct((SLOTS, rows, HEAD) if t else (SLOTS, HEAD, rows), jnp.bfloat16) for t in turned],
        compiler_params=pltpu.CompilerParams(dimension_semantics=("arbitrary",), vmem_limit_bytes=VMEM),
        cost_estimate=pl.CostEstimate(flops=2 * size * D * n, transcendentals=rows, bytes_accessed=2 * (rows * D + n * D * D // 2 + n * size)),
    )(*xs, gain, cos, sin, w)


def _finish(at_ref, x_ref, mine_ref, theirs_ref, w_ref, y_ref, a_s):
    core = at_ref[0]
    for half, ref in ((core, mine_ref), (1 - core, theirs_ref)):
        for m in range(SLOTS):
            a_s[:, pl.ds(pl.multiple_of((4 * half + m) * HEAD, HEAD), HEAD)] = ref[m]
    a = a_s[...]
    wide = D // SLOTS
    for g in range(SLOTS):
        cols = slice(g * wide, (g + 1) * wide)
        y_ref[:, cols] = (x_ref[:, cols].astype(jnp.float32) + _dot(a, w_ref[g], 1, 0)).astype(jnp.bfloat16)


def finish(x, mine, theirs, w, core):
    rows, tb = x.shape[0], 256
    heads = pl.BlockSpec((SLOTS, tb, HEAD), lambda i, _: (0, i, 0))
    return pl.pallas_call(
        _finish,
        grid_spec=pltpu.PrefetchScalarGridSpec(
            num_scalar_prefetch=1,
            grid=(rows // tb,),
            in_specs=[pl.BlockSpec((tb, D), lambda i, _: (i, 0)), heads, heads, pl.BlockSpec((SLOTS, D, D // SLOTS), lambda i, _: (0, 0, 0))],
            out_specs=pl.BlockSpec((tb, D), lambda i, _: (i, 0)),
            scratch_shapes=[pltpu.VMEM((tb, D), jnp.bfloat16)],
        ),
        out_shape=jax.ShapeDtypeStruct(x.shape, x.dtype),
        compiler_params=pltpu.CompilerParams(dimension_semantics=("arbitrary",), vmem_limit_bytes=VMEM),
        cost_estimate=pl.CostEstimate(flops=2 * rows * D * D, transcendentals=0, bytes_accessed=2 * (3 * x.size + D * D)),
    )(jnp.reshape(core, (1,)).astype(jnp.int32), x, mine, theirs, w)


def swap(t):
    return lax.ppermute(t, "sp", [(i, i ^ 1) for i in range(2 * PLANES)])


def up(t, step):
    return lax.ppermute(t, "sp", [(i, i + 2) for i in range(2 * (step - 1), 2 * (PLANES - 1))])


def solution(mesh):
    def step(x, gain, wq, wk, wv, wo):
        own = x.shape[0]
        index, group = lax.axis_index("sp"), lax.axis_index("dp")
        z, core = index // 2, index % 2
        gain = gain.reshape(1, D)
        freq = THETA ** (-jnp.arange(HEAD // 2, dtype=jnp.float32) / (HEAD // 2))

        def angles(chip, first, rows, core):
            place = (chip * 2 + (core ^ jnp.arange(2)[:, None])) * own + first + jnp.arange(rows)[None, :]
            angle = place.reshape(-1).astype(jnp.float32)[:, None] * freq
            return jnp.cos(angle), jnp.sin(angle)

        def after(t, *others):
            return lax.optimization_barrier((t, *others))[0]

        w, here, below = fetch(x, wk, wv, wq)
        sizes = list(zip([sum(CHUNKS[:n]) for n in range(len(CHUNKS))], CHUNKS))
        turns = [[angles(z - s, a, n, 0 if s == 1 and a == 0 else core) for a, n in sizes] for s in range(1, PLANES - 1)]

        def both(t):
            return [t, swap(t)]

        count = len(CHUNKS)
        held = [lax.dynamic_index_in_dim(below, core, keepdims=False)] + [up(after(x[a : a + m], w), 1) for n, (a, m) in enumerate(sizes) if n]
        onward = [up(held[0], 2)]
        k, v, q = project([after(here.reshape(-1, D), held[0])], gain, *angles(z, 0, own, 0), w, (True, False, True))
        half = q.shape[1] // 2
        asked = []
        for n in range(2):
            asked.append(lax.ppermute(q[:, n * half : (n + 1) * half], "sp", [(2 * PLANES - 2, 0), (2 * PLANES - 1, 1)]))

        def answer(n, wait):
            given = after(asked[n], wait)
            shapes = [jax.ShapeDtypeStruct((SLOTS, HEAD, half), jnp.bfloat16), jax.ShapeDtypeStruct((SLOTS, 1, half), jnp.float32)]
            out, stat = lax.cond(
                z == 0,
                lambda t: tuple(flash(t, [(own_k, own_v)], None, 1, part=True)),
                lambda t: tuple(jnp.zeros(a.shape, a.dtype) for a in shapes),
                given,
            )
            back = [(0, 2 * PLANES - 2), (1, 2 * PLANES - 1)]
            outs.append(lax.ppermute(out, "sp", back))
            stats.append(jnp.where(z == PLANES - 1, lax.ppermute(stat, "sp", back), NEG))
            return out

        own_k, own_v, outs, stats = k, v, [], []
        state = flash(q, [(k, v)], None, 1, causal=True)
        quarter = lax.dynamic_slice_in_dim(after(wo, state[1]), group * (D // SLOTS), D // SLOTS, axis=1)
        quarter = lax.all_gather(quarter, "sp", axis=0, tiled=True)
        done = wait = state[1]
        for s in range(1, PLANES - 1):
            seen, keys = (z >= s).astype(jnp.int32), []
            for n in range(count):
                if s == 1 and n == 0:
                    xs = [after(below.reshape(-1, D), done)]
                else:
                    t = after(held[n], wait if n == 0 else state[1])
                    if s < PLANES - 2 and not (s == 1 and n == 0):
                        onward.append(up(t, s + 1))
                    xs = both(t)
                    xs[0] = after(xs[0], done)
                keys.append(project(xs, gain, *turns[s - 1][n], w, (True, False)))
                wait = done = keys[-1][0]
                end = n == count - 1
                if end:
                    if s == 1:
                        w_out = lax.all_gather(after(quarter, done), "dp", axis=0)
                    given = after(q, answer(0, done)) if s == 1 else q
                    state = flash(given, keys, state, seen)
                    done = answer(1, state[1]) if s == 1 else state[1]
            held, onward = onward, []
        seen = merge(state, outs, stats)
        rows = lambda c: lax.dynamic_slice_in_dim(seen, c * own, own, axis=1)
        return finish(x, rows(core), swap(rows(1 - core)), w_out, core)

    tokens, whole = P(("dp", "sp"), None), P("sp", None)
    return jax.shard_map(
        step,
        mesh=mesh,
        in_specs=(tokens, P(None), whole, whole, whole, whole),
        out_specs=tokens,
        check_vma=False,
    )
```

```python
import functools

import jax
import jax.numpy as jnp
from jax import lax
from jax.experimental import pallas as pl
from jax.experimental.pallas import tpu as pltpu
from jax.sharding import PartitionSpec as P


NEG = -1e30
HIDDEN = 2 * NEG
LOG2E = 1.4426950408889634
VMEM = 60 * 2**20
STRIP = 512
BLOCK_Q, BLOCK_K = 512, 1024
HEAD = 256
THETA = 10000
D = 2048
SHARD = 256
PLANES = 4
SLOTS = 4
FIRST = 512
CHUNKS = (512, 512)


def _dot(a, b, ca, cb):
    return lax.dot_general(a, b, (((ca,), (cb,)), ((), ())), preferred_element_type=jnp.float32)


def _flash(pos_ref, q_ref, *rest, pieces_of_keys, causal, start, part, scale, bq, bk):
    pairs, rest = [(rest[2 * n], rest[2 * n + 1]) for n in range(pieces_of_keys)], rest[2 * pieces_of_keys :]
    if not start:
        mix_in, top_in, *rest = rest
    if part:
        o_ref, stat_ref, mix_s, top_s = rest
    else:
        mix_s, top_s = rest
    heads = q_ref.shape[0]
    iq = pl.program_id(0)
    e = scale * LOG2E
    wide = min(STRIP, bq)
    pieces = [(i, at) for i in range(heads) for at in range(0, bq, wide)]
    if start:
        top_s[...] = jnp.full(top_s.shape, NEG, jnp.float32)
        mix_s[...] = jnp.zeros(mix_s.shape, jnp.float32)
    else:
        top_s[...] = top_in[...]
        mix_s[...] = mix_in[...]
    ones = jnp.ones((8, bk), q_ref.dtype)

    def block(k_ref, v_ref, j, masked):
        here = pl.ds(pl.multiple_of(j * bk, bk), bk)
        scores = [_dot(k_ref[i, here, :], q_ref[i, at : at + wide, :], 1, 1) for i, at in pieces]
        weights, keeps = [], []
        for (i, at), s in zip(pieces, scores):
            if masked:
                gap = lax.broadcasted_iota(jnp.int32, (bk, wide), 1) - lax.broadcasted_iota(jnp.int32, (bk, wide), 0)
                s = jnp.where(gap >= j * bk - iq * bq - at, s, HIDDEN)
            old = top_s[i, :, at : at + wide]
            top = jnp.maximum(old, s.max(axis=0, keepdims=True))
            top_s[i, :, at : at + wide] = top
            weights.append(jnp.exp2((s - top) * e).astype(q_ref.dtype))
            keeps.append(jnp.exp2((old - top) * e))
        for (i, at), p, keep in zip(pieces, weights, keeps):
            values = jnp.concatenate([v_ref[i, :, here], ones], axis=0)
            mix_s[i, :, at : at + wide] = mix_s[i, :, at : at + wide] * keep + _dot(values, p, 1, 0)

    for k_ref, v_ref in pairs:
        run = lambda masked, k_ref=k_ref, v_ref=v_ref: lambda j, _: block(k_ref, v_ref, j, masked)
        if causal:
            whole = lax.div(iq * bq, bk)
            lax.fori_loop(0, whole, run(False), None)
            lax.fori_loop(whole, lax.div(iq * bq + bq + bk - 1, bk), run(True), None)
        else:
            lax.fori_loop(0, jnp.where(pos_ref[0] > 0, k_ref.shape[1] // bk, 0), run(False), None)
    if part:
        total = mix_s[:, HEAD : HEAD + 1, :]
        o_ref[...] = (mix_s[:, :HEAD, :] * (1 / total)).astype(o_ref.dtype)
        stat_ref[...] = top_s[...] + jnp.log2(total) * (1 / e)


def _merge(mix_ref, top_ref, *refs, scale, blocks):
    oa_ref, ob_ref, sa_ref, sb_ref, o_ref = refs
    e = scale * LOG2E
    early = pl.program_id(0) < blocks
    top, stat = top_ref[...], jnp.where(early, sa_ref[...], sb_ref[...])
    high = jnp.maximum(top, stat)
    one, two = jnp.exp2((top - high) * e), jnp.exp2((stat - high) * e)
    share = 1 / (mix_ref[:, HEAD : HEAD + 1, :] * one + two)
    one, two = one * share, two * share
    for i in range(o_ref.shape[0]):
        far = jnp.where(early, oa_ref[i], ob_ref[i]).astype(jnp.float32)
        o_ref[i] = (mix_ref[i, :HEAD, :] * one[i] + far * two[i]).T.astype(o_ref.dtype)


def merge(state, outs, stats):
    mix, top = state
    heads, _, sq = mix.shape
    bq = BLOCK_Q
    blocks = outs[0].shape[2] // bq
    first, second = lambda i: (0, 0, jnp.minimum(i, blocks - 1)), lambda i: (0, 0, jnp.maximum(i - blocks, 0))
    return pl.pallas_call(
        functools.partial(_merge, scale=HEAD**-0.5, blocks=blocks),
        grid=(sq // bq,),
        in_specs=[
            pl.BlockSpec((heads, HEAD + 8, bq), lambda i: (0, 0, i)),
            pl.BlockSpec((heads, 1, bq), lambda i: (0, 0, i)),
            pl.BlockSpec((heads, HEAD, bq), first),
            pl.BlockSpec((heads, HEAD, bq), second),
            pl.BlockSpec((heads, 1, bq), first),
            pl.BlockSpec((heads, 1, bq), second),
        ],
        out_specs=pl.BlockSpec((heads, bq, HEAD), lambda i: (0, i, 0)),
        out_shape=jax.ShapeDtypeStruct((heads, sq, HEAD), jnp.bfloat16),
        compiler_params=pltpu.CompilerParams(dimension_semantics=("arbitrary",), vmem_limit_bytes=VMEM),
        cost_estimate=pl.CostEstimate(flops=4 * mix.size, transcendentals=2 * top.size, bytes_accessed=4 * mix.size + 4 * heads * sq * HEAD),
    )(mix, top, *outs, *stats)


def flash(q, keys, state, seen, *, causal=False, part=False):
    heads, sq, d = q.shape
    bq, bk = BLOCK_Q, min([BLOCK_K] + [k.shape[1] for k, _ in keys])
    sk = sum(k.shape[1] for k, _ in keys)
    given, specs = [q], [pl.BlockSpec((heads, bq, d), lambda i, _: (0, i, 0))]
    for pair in keys:
        given += pair
        specs += [pl.BlockSpec(t.shape, lambda i, _: (0, 0, 0)) for t in pair]
    n = len(given)
    state_specs = [pl.BlockSpec((heads, d + 8, bq), lambda i, _: (0, 0, i)), pl.BlockSpec((heads, 1, bq), lambda i, _: (0, 0, i))]
    state_shapes = [jax.ShapeDtypeStruct((heads, d + 8, sq), jnp.float32), jax.ShapeDtypeStruct((heads, 1, sq), jnp.float32)]
    if state is not None:
        given += list(state)
        specs += state_specs
    if part:
        out_specs = [pl.BlockSpec((heads, d, bq), lambda i, _: (0, 0, i)), state_specs[1]]
        out_shape = [jax.ShapeDtypeStruct((heads, d, sq), q.dtype), state_shapes[1]]
        scratch = [pltpu.VMEM((heads, d + 8, bq), jnp.float32), pltpu.VMEM((heads, 1, bq), jnp.float32)]
    else:
        out_specs, out_shape, scratch = state_specs, state_shapes, []
    return pl.pallas_call(
        functools.partial(_flash, pieces_of_keys=len(keys), causal=causal, start=state is None, part=part, scale=d**-0.5, bq=bq, bk=bk),
        grid_spec=pltpu.PrefetchScalarGridSpec(
            num_scalar_prefetch=1, grid=(sq // bq,), in_specs=specs, out_specs=out_specs, scratch_shapes=scratch
        ),
        out_shape=out_shape,
        input_output_aliases={n + 1: 0, n + 2: 1} if state is not None else {},
        compiler_params=pltpu.CompilerParams(dimension_semantics=("arbitrary",), vmem_limit_bytes=VMEM),
        cost_estimate=pl.CostEstimate(
            flops=4 * heads * sq * sk * d // (2 if causal else 1),
            transcendentals=heads * sq * sk,
            bytes_accessed=2 * heads * d * (sq + 2 * sk),
        ),
    )(jnp.reshape(seen, (1,)).astype(jnp.int32), *given)


MESH = pl.DeviceIdType.MESH


def _fetch(*refs):
    n = len(refs) - 15
    x_ref, shards, w_ref, here_ref, below_ref = refs[0], refs[1 : n + 1], *refs[n + 1 : n + 4]
    mine, x_s, load_sem, store_sem, swap_sem, z_send, z_recv, xy_send, xy_recv, x_sem, on_sem = refs[n + 4 :]
    index, g = lax.axis_index("sp"), lax.axis_index("dp")
    z, c = index // 2, index % 2
    rows = lambda plane, core: pl.ds(pl.multiple_of(512 * plane + 256 * core, 256), SHARD)
    part = pl.ds(pl.multiple_of(HEAD * g, HEAD), HEAD)
    line = lambda k: lax.rem(z + k, PLANES)

    loads = [pltpu.make_async_copy(shards[t], mine.at[t], load_sem.at[t]) for t in range(n)]
    loads.append(pltpu.make_async_copy(x_ref, x_s, load_sem.at[n]))
    for load in loads:
        load.start()
    barrier = pltpu.get_barrier_semaphore()
    partners = [(g, 2 * line(k) + core) for k in range(1, PLANES) for core in range(2)] + [(g, 2 * z + 1 - c), (g ^ 1, index), (g ^ 2, index)]
    for device in partners:
        pl.semaphore_signal(barrier, inc=1, device_id=device, device_id_type=MESH)
    pl.semaphore_wait(barrier, len(partners))

    def remote(src, dst, send, recv, device):
        return pltpu.make_async_remote_copy(src_ref=src, dst_ref=dst, send_sem=send, recv_sem=recv, device_id=device, device_id_type=MESH)

    def along(t, k, core):
        cols = pl.ds(pl.multiple_of(4 * HEAD * core + HEAD * g, HEAD), HEAD)
        return remote(mine.at[t, :, cols], w_ref.at[t, rows(z, c), part], z_send.at[t, k - 1, core], z_recv.at[t, k - 1, c], (g, 2 * line(k) + core))

    def arrived(t, k, s):
        spot = w_ref.at[t, rows(line(PLANES - k), s), part]
        remote(spot, spot, z_send.at[t, k - 1, 0], z_recv.at[t, k - 1, s], (g, 2 * line(k))).wait_recv()

    def across(t, k, s, quarter, to, slot):
        q = pl.ds(pl.multiple_of(HEAD * (g ^ quarter), HEAD), HEAD)
        spot = w_ref.at[t, rows(line(PLANES - k), s), q]
        return remote(spot, spot, xy_send.at[t, k - 1, s, slot], xy_recv.at[t, k - 1, s, slot], (g ^ to, index))

    sends_on = {1: z == 2, 2: (z == 1) | (z == 2), 3: z == 1}
    straight = {1: z != 3, 2: (z == 0) | (z == 3), 3: z != 0}

    def further(t, k, s):
        spot = w_ref.at[t, rows(line(PLANES - k), s), part]
        step = 2 * z - 3
        return remote(spot, spot, on_sem.at[t, k - 1, s], z_recv.at[t, lax.rem(k + step + PLANES, PLANES) - 1, s], (g, 2 * (z + step) + c))

    sent, stores = [], []
    pieces = [(t, k, s) for t in range(n) for k in range(1, PLANES) for s in range(2)]
    for t in range(n):
        loads[t].wait()
        for k in range(1, PLANES):
            for core in range(2):
                pl.when(straight[k])(along(t, k, core).start)
        theirs = pl.ds(pl.multiple_of(4 * HEAD * (1 - c), 4 * HEAD), 4 * HEAD)
        ours = pl.ds(pl.multiple_of(4 * HEAD * c, 4 * HEAD), 4 * HEAD)
        other = remote(mine.at[t, :, theirs], w_ref.at[t, rows(z, c), :], swap_sem.at[t, 0], swap_sem.at[t, 1], (g, 2 * z + 1 - c))
        other.start()
        sent.append(other)
        stores.append(pltpu.make_async_copy(mine.at[t, :, ours], w_ref.at[t, rows(z, c), :], store_sem.at[t]))
        stores[-1].start()

    loads[n].wait()
    other = (g, 2 * z + 1 - c)
    stores.append(pltpu.make_async_copy(x_s, here_ref.at[c], store_sem.at[n]))
    stores[-1].start()
    sent.append(remote(x_s, here_ref.at[c], x_sem.at[0, 0], x_sem.at[0, 1], other))
    sent[-1].start()
    rise = remote(x_s.at[pl.ds(0, FIRST)], below_ref.at[c], x_sem.at[1, 0], x_sem.at[1, 1], (g, 2 * line(1) + c))
    pl.when(z < PLANES - 2)(rise.start)

    def relay(t, k, s):
        came, to = (2, 1) if s == 0 else (1, 2)
        across(t, k, s, came, came, came - 1).wait_recv()
        sent.append(across(t, k, s, came, to, 2))
        sent[-1].start()

    lag = 2
    for i, piece in enumerate(pieces):
        arrived(*piece)
        pl.when(sends_on[piece[1]])(further(*piece).start)
        for to in (1, 2):
            sent.append(across(*piece, 0, to, to - 1))
            sent[-1].start()
        if i >= lag:
            relay(*pieces[i - lag])
    pl.when(z == PLANES - 2)(rise.start)
    for piece in pieces[len(pieces) - lag :]:
        relay(*piece)
    for t, k, s in pieces:
        stays = 1 if s == 0 else 2
        across(t, k, s, stays, stays, stays - 1).wait_recv()
        across(t, k, s, 3, 3, 2).wait_recv()
    for t in range(n):
        spot = w_ref.at[t, rows(z, 1 - c), :]
        remote(spot, spot, swap_sem.at[t, 0], swap_sem.at[t, 1], (g, 2 * z + 1 - c)).wait_recv()
        stores[t].wait()
    stores[n].wait()
    remote(here_ref.at[1 - c], here_ref.at[1 - c], x_sem.at[0, 0], x_sem.at[0, 1], other).wait_recv()

    @pl.when(z > 0)
    def _():
        rise.wait_recv()
        spot = below_ref.at[c]
        on = remote(spot, spot, x_sem.at[2, 0], x_sem.at[2, 1], other)
        on.start()
        spot = below_ref.at[1 - c]
        remote(spot, spot, x_sem.at[2, 0], x_sem.at[2, 1], other).wait_recv()
        on.wait_send()

    pl.when(z < PLANES - 1)(rise.wait_send)
    for t, k, s in pieces:
        pl.when(sends_on[k])(further(t, k, s).wait_send)
        pl.when(straight[k])(along(t, k, s).wait_send)
    for copy in sent:
        copy.wait_send()


def fetch(x, *shards):
    n = len(shards)
    dma = pltpu.SemaphoreType.DMA
    return pl.pallas_call(
        _fetch,
        in_specs=[pl.BlockSpec(memory_space=pl.ANY)] * (n + 1),
        out_specs=[pl.BlockSpec(memory_space=pl.ANY)] * 3,
        out_shape=[
            jax.ShapeDtypeStruct((n, D, D // 2), jnp.bfloat16),
            jax.ShapeDtypeStruct((2, *x.shape), jnp.bfloat16),
            jax.ShapeDtypeStruct((2, FIRST, D), jnp.bfloat16),
        ],
        scratch_shapes=[
            pltpu.VMEM((n, SHARD, D), jnp.bfloat16),
            pltpu.VMEM(x.shape, jnp.bfloat16),
            dma((n + 1,)),
            dma((n + 1,)),
            dma((n, 2)),
            dma((n, 3, 2)),
            dma((n, 3, 2)),
            dma((n, 3, 2, 3)),
            dma((n, 3, 2, 3)),
            dma((3, 2)),
            dma((n, 3, 2)),
        ],
        compiler_params=pltpu.CompilerParams(collective_id=0, has_side_effects=True, vmem_limit_bytes=VMEM),
        cost_estimate=pl.CostEstimate(flops=10**11, transcendentals=0, bytes_accessed=10**7),
    )(x, *shards)


def _project(*refs, parts, blocks, turned):
    *xs, gain_ref, cos_ref, sin_ref, w_ref = refs[: parts + 4]
    outs = refs[parts + 4 :]
    wide = xs[0][...] if parts == 1 else jnp.where(pl.program_id(0) < blocks, xs[0][...], xs[1][...])
    wide = wide.astype(jnp.float32)
    scale = lax.rsqrt(jnp.mean(wide * wide, -1, keepdims=True) + 1e-6)
    a = (wide * scale * gain_ref[...].astype(jnp.float32)).astype(jnp.bfloat16)
    cos, sin = cos_ref[...], sin_ref[...]
    half = HEAD // 2
    for t, o in enumerate(outs):
        y = _dot(a, w_ref[t], 1, 0).astype(jnp.bfloat16)
        for m in range(SLOTS):
            part = y[:, m * HEAD : (m + 1) * HEAD]
            if turned[t]:
                lo, hi = part[:, :half].astype(jnp.float32), part[:, half:].astype(jnp.float32)
                o[m, :, :half] = (lo * cos - hi * sin).astype(jnp.bfloat16)
                o[m, :, half:] = (hi * cos + lo * sin).astype(jnp.bfloat16)
            else:
                o[m] = part.T


def project(xs, gain, cos, sin, w, turned):
    part = xs[0].shape[0]
    rows, tb, n = part * len(xs), min(512, part), len(turned)
    blocks = part // tb
    if len(xs) == 1:
        specs = [pl.BlockSpec((tb, D), lambda i: (i, 0))]
    else:
        specs = [pl.BlockSpec((tb, D), lambda i: (jnp.minimum(i, blocks - 1), 0)), pl.BlockSpec((tb, D), lambda i: (jnp.maximum(i - blocks, 0), 0))]
    size = SLOTS * rows * HEAD
    return pl.pallas_call(
        functools.partial(_project, parts=len(xs), blocks=blocks, turned=turned),
        grid=(rows // tb,),
        in_specs=specs
        + [
            pl.BlockSpec((1, D), lambda i: (0, 0)),
            pl.BlockSpec((tb, HEAD // 2), lambda i: (i, 0)),
            pl.BlockSpec((tb, HEAD // 2), lambda i: (i, 0)),
            pl.BlockSpec((n, D, D // 2), lambda i: (0, 0, 0), pipeline_mode=pl.Buffered(1)),
        ],
        out_specs=[pl.BlockSpec((SLOTS, tb, HEAD), lambda i: (0, i, 0)) if t else pl.BlockSpec((SLOTS, HEAD, tb), lambda i: (0, 0, i)) for t in turned],
        out_shape=[jax.ShapeDtypeStruct((SLOTS, rows, HEAD) if t else (SLOTS, HEAD, rows), jnp.bfloat16) for t in turned],
        compiler_params=pltpu.CompilerParams(dimension_semantics=("arbitrary",), vmem_limit_bytes=VMEM),
        cost_estimate=pl.CostEstimate(flops=2 * size * D * n, transcendentals=rows, bytes_accessed=2 * (rows * D + n * D * D // 2 + n * size)),
    )(*xs, gain, cos, sin, w)


def _finish(at_ref, x_ref, mine_ref, theirs_ref, w_ref, y_ref, a_s):
    core = at_ref[0]
    for half, ref in ((core, mine_ref), (1 - core, theirs_ref)):
        for m in range(SLOTS):
            a_s[:, pl.ds(pl.multiple_of((4 * half + m) * HEAD, HEAD), HEAD)] = ref[m]
    a = a_s[...]
    wide = D // SLOTS
    for g in range(SLOTS):
        cols = slice(g * wide, (g + 1) * wide)
        y_ref[:, cols] = (x_ref[:, cols].astype(jnp.float32) + _dot(a, w_ref[g], 1, 0)).astype(jnp.bfloat16)


def finish(x, mine, theirs, w, core):
    rows, tb = x.shape[0], 256
    heads = pl.BlockSpec((SLOTS, tb, HEAD), lambda i, _: (0, i, 0))
    return pl.pallas_call(
        _finish,
        grid_spec=pltpu.PrefetchScalarGridSpec(
            num_scalar_prefetch=1,
            grid=(rows // tb,),
            in_specs=[pl.BlockSpec((tb, D), lambda i, _: (i, 0)), heads, heads, pl.BlockSpec((SLOTS, D, D // SLOTS), lambda i, _: (0, 0, 0))],
            out_specs=pl.BlockSpec((tb, D), lambda i, _: (i, 0)),
            scratch_shapes=[pltpu.VMEM((tb, D), jnp.bfloat16)],
        ),
        out_shape=jax.ShapeDtypeStruct(x.shape, x.dtype),
        compiler_params=pltpu.CompilerParams(dimension_semantics=("arbitrary",), vmem_limit_bytes=VMEM),
        cost_estimate=pl.CostEstimate(flops=2 * rows * D * D, transcendentals=0, bytes_accessed=2 * (3 * x.size + D * D)),
    )(jnp.reshape(core, (1,)).astype(jnp.int32), x, mine, theirs, w)


def swap(t):
    return lax.ppermute(t, "sp", [(i, i ^ 1) for i in range(2 * PLANES)])


def up(t, step):
    return lax.ppermute(t, "sp", [(i, i + 2) for i in range(2 * (step - 1), 2 * (PLANES - 1))])


def solution(mesh):
    def step(x, gain, wq, wk, wv, wo):
        own = x.shape[0]
        index, group = lax.axis_index("sp"), lax.axis_index("dp")
        z, core = index // 2, index % 2
        gain = gain.reshape(1, D)
        freq = THETA ** (-jnp.arange(HEAD // 2, dtype=jnp.float32) / (HEAD // 2))

        def angles(chip, first, rows, core):
            place = (chip * 2 + (core ^ jnp.arange(2)[:, None])) * own + first + jnp.arange(rows)[None, :]
            angle = place.reshape(-1).astype(jnp.float32)[:, None] * freq
            return jnp.cos(angle), jnp.sin(angle)

        def after(t, *others):
            return lax.optimization_barrier((t, *others))[0]

        w, here, below = fetch(x, wk, wv, wq)
        sizes = list(zip([sum(CHUNKS[:n]) for n in range(len(CHUNKS))], CHUNKS))
        turns = [[angles(z - s, a, n, 0 if s == 1 and a == 0 else core) for a, n in sizes] for s in range(1, PLANES - 1)]

        def both(t):
            return [t, swap(t)]

        count = len(CHUNKS)
        held = [lax.dynamic_index_in_dim(below, core, keepdims=False)] + [up(after(x[a : a + m], w), 1) for n, (a, m) in enumerate(sizes) if n]
        onward = [up(held[0], 2)]
        k, v, q = project([after(here.reshape(-1, D), held[0])], gain, *angles(z, 0, own, 0), w, (True, False, True))
        half = q.shape[1] // 2
        asked = []
        for n in range(2):
            asked.append(lax.ppermute(q[:, n * half : (n + 1) * half], "sp", [(2 * PLANES - 2, 0), (2 * PLANES - 1, 1)]))

        def answer(n, wait):
            given = after(asked[n], wait)
            shapes = [jax.ShapeDtypeStruct((SLOTS, HEAD, half), jnp.bfloat16), jax.ShapeDtypeStruct((SLOTS, 1, half), jnp.float32)]
            out, stat = lax.cond(
                z == 0,
                lambda t: tuple(flash(t, [(own_k, own_v)], None, 1, part=True)),
                lambda t: tuple(jnp.zeros(a.shape, a.dtype) for a in shapes),
                given,
            )
            back = [(0, 2 * PLANES - 2), (1, 2 * PLANES - 1)]
            outs.append(lax.ppermute(out, "sp", back))
            stats.append(jnp.where(z == PLANES - 1, lax.ppermute(stat, "sp", back), NEG))
            return out

        own_k, own_v, outs, stats = k, v, [], []
        state = flash(q, [(k, v)], None, 1, causal=True)
        quarter = lax.dynamic_slice_in_dim(after(wo, state[1]), group * (D // SLOTS), D // SLOTS, axis=1)
        quarter = lax.all_gather(quarter, "sp", axis=0, tiled=True)
        done = wait = state[1]
        for s in range(1, PLANES - 1):
            seen, keys = (z >= s).astype(jnp.int32), []
            for n in range(count):
                if s == 1 and n == 0:
                    xs = [after(below.reshape(-1, D), done)]
                else:
                    t = after(held[n], wait if n == 0 else state[1])
                    if s < PLANES - 2 and not (s == 1 and n == 0):
                        onward.append(up(t, s + 1))
                    xs = both(t)
                    xs[0] = after(xs[0], done)
                keys.append(project(xs, gain, *turns[s - 1][n], w, (True, False)))
                wait = done = keys[-1][0]
                end = n == count - 1
                if end or s > 1:
                    if s == 1:
                        w_out = lax.all_gather(after(quarter, done), "dp", axis=0)
                    given = after(q, answer(0, done)) if s == 1 else q
                    state = flash(given, keys, state, seen)
                    keys, done = [], answer(1, state[1]) if s == 1 else state[1]
            held, onward = onward, []
        seen = merge(state, outs, stats)
        rows = lambda c: lax.dynamic_slice_in_dim(seen, c * own, own, axis=1)
        return finish(x, rows(core), swap(rows(1 - core)), w_out, core)

    tokens, whole = P(("dp", "sp"), None), P("sp", None)
    return jax.shard_map(
        step,
        mesh=mesh,
        in_specs=(tokens, P(None), whole, whole, whole, whole),
        out_specs=tokens,
        check_vma=False,
    )
```
